32 devices in a mesh: angle: 8 (over y, x, core), scan: 4 (over z).
Axes of the slice: x: 2, y: 2, z: 4, core: 2. Of those that a mesh axis runs over, the one named last changes fastest.
Arguments:
- object_slices: float32 [2, 3, 256, 512], P(None, None, 'scan', 'angle'), may hold values from -5 to 5
- probe: float32 [2, 128, 128], replicated, may hold values from -6 to 6
- intensities: float32 [8, 4, 2, 128, 128], P('angle', 'scan'), may hold values from 0.5 to 3.5
- row_offsets: int32 [8, 4, 2], P('angle', 'scan'), may hold values from 0 to 64
- column_starts: int32 [8, 4, 2], P('angle', 'scan'), may hold values from 0 to 320
- slice_shifts: int32 [8, 3], P('angle'), may hold values from 0 to 64
- counts: int32 [8, 4], P('angle', 'scan'), may hold values from 1 to 2, as said below
Outputs:
- object_gradient: float32 [2, 3, 256, 512], P(None, None, 'scan', 'angle')
- probe_gradient: float32 [2, 128, 128], replicated
The draws below stay inside these ranges and needn't reach their ends.
Inputs may be any that keep to these rules, and one draw needn't show every extreme that they name: `counts`: the largest value 2 occurs in every draw.
All inputs are finite; a program needn't handle non-finite values.
Results may differ from the reference program's by a relative error of at most 0.0003.
Values sent between devices are 32-bit elements; how exact they have to be, the bound alone decides.
A program may use at most 64 MiB of HBM per device.

```python
import jax
import jax.numpy as jnp
from jax import lax

PATCH = 128
LAYERS = 3
COLUMNS = 512
TILT = 64
BAND = 64
SLOTS = 2
ANGLES = 8
SCANS = 4
ROWS = 256
N_ANGLE = 8
N_SCAN = 4


def draw_counts(key, part):
    first, second, third, fourth = jax.random.split(jax.random.fold_in(key, 17), 4)
    lefthand = jax.random.randint(first, (ANGLES, SCANS), 0, SLOTS)
    righthand = jax.random.randint(second, (ANGLES, SCANS), 0, SLOTS)
    values = SLOTS // 3 + 1 + lefthand * righthand // (2 * (SLOTS - 1))
    which_row = jax.random.randint(third, (), 0, ANGLES)
    which_column = jax.random.randint(fourth, (), 0, SCANS)
    return values.at[which_row, which_column].set(SLOTS).astype(jnp.int32)


def touch_ends(values, key, low, top_value):
    index_at = [jax.random.randint(jax.random.fold_in(key, axis), (), 0, length) for axis, length in enumerate(values.shape)]
    main_axis = values.shape.index(max(values.shape))
    next_to = index_at[:main_axis] + [(index_at[main_axis] + 1) % values.shape[main_axis]] + index_at[main_axis + 1:]
    return values.at[tuple(index_at)].set(low).at[tuple(next_to)].set(top_value)


def shard_levels(key, shape, cuts, least, high):
    gain = 1.0
    for axis_at, shards_of in cuts:
        steps = jax.random.uniform(jax.random.fold_in(jax.random.fold_in(key, 6), axis_at), (shards_of,), jnp.float32, least / len(cuts), high / len(cuts))
        gain = gain * jnp.repeat(jnp.exp(steps), shape[axis_at] // shards_of).reshape((-1,) + (1,) * (len(shape) - 1 - axis_at))
    return gain


def bell_draw(key, extent, spread, limit, pieces=(), kind=jnp.bfloat16):
    array = spread * jax.random.normal(key, extent, jnp.float32)
    if pieces:
        array = array * shard_levels(key, extent, pieces, -0.22, 0.18)
    return jnp.clip(array, -limit, limit).astype(kind)


def setup_inputs(seed: int = 0) -> dict:
    key_of = jax.random.split(jax.random.key(seed), 8)
    return {
        "object_slices": bell_draw(key_of[0], (2, LAYERS, ROWS, COLUMNS), 0.7, 5.0, ((2, 4), (3, 8)), jnp.float32),
        "probe": bell_draw(key_of[1], (2, PATCH, PATCH), 1.0, 6.0, (), jnp.float32),
        "intensities": jnp.clip(0.5 + 3.0 * jax.random.uniform(key_of[2], (ANGLES, SCANS, SLOTS, PATCH, PATCH), jnp.float32) ** shard_levels(key_of[2], (ANGLES, SCANS, SLOTS, PATCH, PATCH), ((0, 8), (1, 4)), -0.2, 0.2), 0.5, 3.5),
        "row_offsets": touch_ends(jax.random.randint(key_of[3], (ANGLES, SCANS, SLOTS), 0, 3 * BAND - PATCH + 1), jax.random.fold_in(key_of[3], 1), 0, 3 * BAND - PATCH).astype(jnp.int32),
        "column_starts": touch_ends(jax.random.randint(key_of[4], (ANGLES, SCANS, SLOTS), 0, COLUMNS - PATCH - TILT + 1), jax.random.fold_in(key_of[4], 1), 0, COLUMNS - PATCH - TILT).astype(jnp.int32),
        "slice_shifts": touch_ends(jax.random.randint(key_of[5], (ANGLES, LAYERS), 0, TILT + 1), jax.random.fold_in(key_of[5], 1), 0, TILT).astype(jnp.int32),
        "counts": draw_counts(jax.random.fold_in(key_of[7], 71), 0),
    }


def propagator(size):
    index = jnp.arange(size, dtype=jnp.int32)
    centred = ((index + size // 2) % size - size // 2).astype(jnp.float32)
    radius = centred[:, None] * centred[:, None] + centred[None, :] * centred[None, :]
    phase = 8.0 * jnp.pi * radius / (size * size)
    return (jnp.cos(phase), jnp.sin(phase))

def patch_loss(slab, probe, measured, weight):
    size = probe.shape[1]
    kern_re, kern_im = propagator(size)
    kernel = kern_re + 1j * kern_im
    wave = probe[0] + 1j * probe[1]
    layers = slab.shape[1]
    for k in range(layers):
        wave = wave * (slab[0, k] + 1j * slab[1, k])
        if k + 1 < layers:
            wave = jnp.fft.ifft2(kernel * jnp.fft.fft2(wave, norm='ortho'), norm='ortho')
    far = jnp.fft.fft2(wave, norm='ortho')
    power = jnp.real(far) * jnp.real(far) + jnp.imag(far) * jnp.imag(far)
    differ = power - measured
    return weight * jnp.sum(differ * differ)

def reference(object_slices, probe, intensities, row_offsets, column_starts, slice_shifts, counts):
    layers = object_slices.shape[1]
    rows = object_slices.shape[2]
    band = rows // N_SCAN
    size = probe.shape[1]
    slots = row_offsets.shape[2]
    padded = jnp.pad(object_slices, ((0, 0), (0, 0), (band, band), (0, 0)))
    total = N_ANGLE * N_SCAN * slots

    def visit(carry, index):
        gradient_object, gradient_probe = carry
        angle = index // (N_SCAN * slots)
        scanned = index // slots % N_SCAN
        slot = index % slots
        top = (scanned * band + row_offsets[angle, scanned, slot]).astype(jnp.int32)
        start = column_starts[angle, scanned, slot].astype(jnp.int32)
        shifts = slice_shifts[angle]
        zero = jnp.zeros((), jnp.int32)
        slab = jnp.concatenate([lax.dynamic_slice(padded, (zero, zero + k, top, start + shifts[k]), (2, 1, size, size)) for k in range(layers)], axis=1)
        weight = jnp.where(slot < counts[angle, scanned], 0.5 / N_ANGLE, 0.0).astype(jnp.float32)
        measured = intensities[angle, scanned, slot]
        loss, pull = jax.vjp(lambda s, p: patch_loss(s, p, measured, weight), slab, probe)
        slab_grad, probe_grad = pull(jnp.ones_like(loss))
        for k in range(layers):
            place = (zero, zero + k, top, start + shifts[k])
            current = lax.dynamic_slice(gradient_object, place, (2, 1, size, size))
            gradient_object = lax.dynamic_update_slice(gradient_object, current + slab_grad[:, k:k + 1], place)
        return ((gradient_object, gradient_probe + probe_grad), None)
    start_carry = (jnp.zeros(padded.shape, jnp.float32), jnp.zeros(probe.shape, jnp.float32))
    (gradient_object, gradient_probe), unused = lax.scan(visit, start_carry, jnp.arange(total, dtype=jnp.int32))
    return (gradient_object[:, :, band:band + rows], gradient_probe)
```

```python
from functools import partial

import jax
import jax.numpy as jnp
import ml_dtypes
import numpy as np
from jax import lax
from jax.experimental import pallas as pl
from jax.experimental.pallas import tpu as pltpu
from jax.sharding import PartitionSpec as P


def shifted(cells, axis, step):
    count = lax.axis_size(axis)
    ends = count - 1
    if step > 0:
        pairs = [(i, (i + 1) % count) for i in range(ends)]
    else:
        pairs = [((i + 1) % count, i) for i in range(ends)]
    return lax.ppermute(cells, axis, pairs)


def operators(size):
    index = np.arange(size)
    turns = np.outer(index, index) % size
    fourier = np.exp(-2j * np.pi * turns / size) / np.sqrt(size)
    centred = (index + size // 2) % size - size // 2
    factor = np.exp(8j * np.pi * centred**2 / size**2)
    step = np.conj(fourier) @ (factor[:, None] * fourier)
    packed = []
    for matrix in (step, fourier):
        right = np.block([[matrix.real, matrix.imag], [-matrix.imag, matrix.real]])
        packed.append(right)
        packed.append(right.T)
    out = np.zeros((4, 2, 2 * size, 2 * size), ml_dtypes.bfloat16)
    for i, matrix in enumerate(packed):
        whole = matrix.astype(np.float32)
        high = whole.astype(ml_dtypes.bfloat16)
        out[i, 0] = high
        out[i, 1] = (whole - high.astype(np.float32)).astype(ml_dtypes.bfloat16)
    return out


def halves(x):
    high = x.astype(jnp.bfloat16)
    return high, (x - high.astype(jnp.float32)).astype(jnp.bfloat16)


def dot(a, b):
    return jnp.dot(a, b, preferred_element_type=jnp.float32)


def both_sides(waves, right, left):
    size = waves[0][0].shape[0]
    stacked = jnp.concatenate([jnp.concatenate([re, im], axis=1) for re, im in waves], axis=0)
    high, low = halves(stacked)
    out = dot(high, right[0]) + (dot(low, right[0]) + dot(high, right[1]))
    rows = [out[s * size : (s + 1) * size] for s in range(len(waves))]
    beside = jnp.concatenate(
        [
            jnp.concatenate([r[:, :size] for r in rows], axis=1),
            jnp.concatenate([r[:, size:] for r in rows], axis=1),
        ],
        axis=0,
    )
    high, low = halves(beside)
    out = dot(left[0], high) + (dot(left[0], low) + dot(left[1], high))
    return [
        (out[:size, s * size : (s + 1) * size], out[size:, s * size : (s + 1) * size])
        for s in range(len(waves))
    ]


def times(a, b):
    return (a[0] * b[0] - a[1] * b[1], a[0] * b[1] + a[1] * b[0])


def conj_times(a, b):
    return (a[0] * b[0] + a[1] * b[1], a[0] * b[1] - a[1] * b[0])


def compute_kernel(
    angles, rows_ref, cols_ref, shifts_ref, counts_ref, region_ref, probe_ref, measured_ref, mats_ref,
    grad_ref, probe_grad_ref,
):
    blocks, layers, height, lanes = region_ref.shape
    width = lanes // 2
    size = probe_ref.shape[1]
    slots = measured_ref.shape[0]
    lane = lax.broadcasted_iota(jnp.int32, (size, lanes), 1)
    lower = lane < width
    swap = lambda x: pltpu.roll(x, width, 1)
    tops = [rows_ref[s] for s in range(slots)]
    starts = [[cols_ref[s] + shifts_ref[k] for k in range(layers)] for s in range(slots)]

    def place(s, k):
        q = starts[s][k] // width
        return q, starts[s][k] - q * width

    def patch(s, k):
        q, r = place(s, k)
        rows = pl.ds(tops[s], size)
        first = region_ref[q, k, rows, :]
        second = region_ref[q + 1, k, rows, :]
        third = region_ref[jnp.minimum(q + 2, blocks - 1), k, rows, :]
        back = lax.rem(lanes - r, lanes)
        inside = lane < lanes - r
        pieces = []
        for near, far in (
            (jnp.where(lower, first, swap(second)), third),
            (jnp.where(lower, swap(first), second), swap(third)),
        ):
            pieces.append(jnp.where(inside, pltpu.roll(near, back, 1), pltpu.roll(far, back, 1)))
        return tuple(pieces)

    objects = [[patch(s, k) for k in range(layers)] for s in range(slots)]
    step_r, step_l, four_r, four_l = [(mats_ref[i, 0], mats_ref[i, 1]) for i in range(4)]
    waves = [(probe_ref[0], probe_ref[1])] * slots
    before = []
    for k in range(layers):
        before.append(waves)
        waves = [times(waves[s], objects[s][k]) for s in range(slots)]
        if k + 1 < layers:
            waves = both_sides(waves, step_r, step_l)
    far = both_sides(waves, four_r, four_l)
    grads = []
    for s in range(slots):
        weight = jnp.where(s < counts_ref[0], 2.0 / angles, 0.0)
        re, im = far[s]
        scale = weight * (re * re + im * im - measured_ref[s])
        grads.append((scale * re, scale * im))
    grads = both_sides(grads, four_l, four_r)
    grad_ref[...] = jnp.zeros(grad_ref.shape, jnp.float32)
    for k in reversed(range(layers)):
        for s in range(slots):
            re, im = conj_times(before[k][s], grads[s])
            q, r = place(s, k)
            rows = pl.ds(tops[s], size)
            re, im = pltpu.roll(re, r, 1), pltpu.roll(im, r, 1)
            zero = jnp.zeros_like(re)
            near_re, near_im = jnp.where(lane >= r, re, zero), jnp.where(lane >= r, im, zero)
            far_re, far_im = jnp.where(lane < r, re, zero), jnp.where(lane < r, im, zero)
            grad_ref[q, k, rows, :] += jnp.where(lower, near_re, swap(near_im))
            grad_ref[q + 1, k, rows, :] += jnp.where(lower, swap(near_re), near_im)
            last = jnp.minimum(q + 2, blocks - 1)
            grad_ref[last, k, rows, :] += jnp.where(lower, far_re, swap(far_im))
        grads = [conj_times(objects[s][k], grads[s]) for s in range(slots)]
        if k > 0:
            grads = both_sides(grads, step_l, step_r)
    probe_grad_ref[0] = sum(g[0] for g in grads)
    probe_grad_ref[1] = sum(g[1] for g in grads)


def gradients(region, probe, intensities, row_offsets, column_starts, slice_shifts, counts):
    angles = lax.axis_size("angle")
    smem = pl.BlockSpec(memory_space=pltpu.SMEM)
    vmem = pl.BlockSpec(memory_space=pltpu.VMEM)
    return pl.pallas_call(
        partial(compute_kernel, angles),
        out_shape=(
            jax.ShapeDtypeStruct(region.shape, jnp.float32),
            jax.ShapeDtypeStruct(probe.shape, jnp.float32),
        ),
        in_specs=[smem] * 4 + [vmem] * 4,
        out_specs=(vmem, vmem),
        compiler_params=pltpu.CompilerParams(vmem_limit_bytes=48 * 2**20),
    )(
        row_offsets.reshape(-1), column_starts.reshape(-1), slice_shifts.reshape(-1),
        counts.reshape(-1), region, probe, intensities[0, 0], jnp.asarray(operators(probe.shape[1])),
    )


def padded(cells, sides, width):
    for axis, dim in sides:
        count = lax.axis_size(axis)
        ends = count - 1
        head = lax.slice_in_dim(cells, 0, width, axis=dim)
        tail = lax.slice_in_dim(cells, cells.shape[dim] - width, cells.shape[dim], axis=dim)
        cells = jnp.concatenate(
            [
                lax.ppermute(tail, axis, [(i, (i + 1) % count) for i in range(ends)]),
                cells,
                lax.ppermute(head, axis, [((i + 1) % count, i) for i in range(ends)]),
            ],
            axis=dim,
        )
    return cells


def propagator(size):
    index = jnp.arange(size, dtype=jnp.int32)
    centred = ((index + size // 2) % size - size // 2).astype(jnp.float32)
    radius = centred[:, None] * centred[:, None] + centred[None, :] * centred[None, :]
    phase = 8.0 * jnp.pi * radius / (size * size)
    return (jnp.cos(phase), jnp.sin(phase))


def tables(size):
    index = jnp.arange(size, dtype=jnp.int32)
    turns = index[:, None] * index[None, :] % size
    phase = 2.0 * jnp.pi * turns.astype(jnp.float32) / size
    scale = 1.0 / jnp.sqrt(jnp.float32(size))
    return (jnp.cos(phase) * scale, jnp.sin(phase) * scale)


def matmul(first, second):
    return jnp.dot(
        first, second, precision=lax.Precision.HIGHEST, preferred_element_type=jnp.float32
    )


def transform(real_part, imag_part, cosine, sine, sign):
    left_re = matmul(cosine, real_part) - sign * matmul(sine, imag_part)
    left_im = matmul(cosine, imag_part) + sign * matmul(sine, real_part)
    right_re = matmul(left_re, cosine) - sign * matmul(left_im, sine)
    right_im = matmul(left_im, cosine) + sign * matmul(left_re, sine)
    return (right_re, right_im)


def local_loss(slab, probe, measured, weight, cosine, sine, kern_re, kern_im):
    wave_re, wave_im = (probe[0], probe[1])
    layers = slab.shape[1]
    for k in range(layers):
        object_re, object_im = (slab[0, k], slab[1, k])
        wave_re, wave_im = (
            wave_re * object_re - wave_im * object_im,
            wave_re * object_im + wave_im * object_re,
        )
        if k + 1 < layers:
            freq_re, freq_im = transform(wave_re, wave_im, cosine, sine, -1.0)
            freq_re, freq_im = (
                freq_re * kern_re - freq_im * kern_im,
                freq_re * kern_im + freq_im * kern_re,
            )
            wave_re, wave_im = transform(freq_re, freq_im, cosine, sine, 1.0)
    far_re, far_im = transform(wave_re, wave_im, cosine, sine, -1.0)
    differ = far_re * far_re + far_im * far_im - measured
    return weight * jnp.sum(differ * differ)


def general(object_slices, probe, intensities, row_offsets, column_starts, slice_shifts, counts):
    band = object_slices.shape[2]
    framed = padded(object_slices, (("scan", 2),), band)
    region = lax.all_gather(framed, "angle", axis=3, tiled=True)
    size = probe.shape[1]
    slots = row_offsets.shape[2]
    layers = region.shape[1]
    angles = lax.axis_size("angle")
    cosine, sine = tables(size)
    kern_re, kern_im = propagator(size)
    shifts = slice_shifts[0]
    zero = jnp.zeros((), jnp.int32)

    def visit(slot, carry):
        gradient_region, gradient_probe = carry
        top = row_offsets[0, 0, slot]
        start = column_starts[0, 0, slot]
        slab = jnp.concatenate(
            [
                lax.dynamic_slice(
                    region, (zero, zero + k, top, start + shifts[k]), (2, 1, size, size)
                )
                for k in range(layers)
            ],
            axis=1,
        )
        weight = jnp.where(slot < counts[0, 0], 0.5 / angles, 0.0).astype(jnp.float32)
        measured = intensities[0, 0, slot]
        scorer = partial(
            local_loss,
            measured=measured,
            weight=weight,
            cosine=cosine,
            sine=sine,
            kern_re=kern_re,
            kern_im=kern_im,
        )
        loss, pull = jax.vjp(scorer, slab, probe)
        slab_grad, probe_grad = pull(jnp.ones_like(loss))
        for k in range(layers):
            place = (zero, zero + k, top, start + shifts[k])
            current = lax.dynamic_slice(gradient_region, place, (2, 1, size, size))
            gradient_region = lax.dynamic_update_slice(
                gradient_region, current + slab_grad[:, k : k + 1], place
            )
        return (gradient_region, gradient_probe + probe_grad)

    start_carry = (jnp.zeros(region.shape, jnp.float32), jnp.zeros(probe.shape, jnp.float32))
    gradient_region, gradient_probe = lax.fori_loop(0, slots, visit, start_carry)
    shared = lax.psum_scatter(gradient_region, "angle", scatter_dimension=3, tiled=True)
    edges = jnp.concatenate([shared[:, :, :band], shared[:, :, 2 * band :]], axis=2)
    rimmed = padded(edges, (("scan", 2),), band)
    object_gradient = shared[:, :, band : 2 * band] + rimmed[:, :, :band] + rimmed[:, :, 3 * band :]
    group_total = lax.psum(gradient_probe, "scan")
    probe_gradient = lax.psum(group_total, "angle")
    return (object_gradient, probe_gradient)


def packable(object_slices, probe):
    size = probe.shape[1]
    band, width = object_slices.shape[2:]
    return 2 * width == size == 128 and band % 8 == 0 and lax.axis_size("angle") >= 4


def local(object_slices, probe, intensities, row_offsets, column_starts, slice_shifts, counts):
    args = (object_slices, probe, intensities, row_offsets, column_starts, slice_shifts, counts)
    if not packable(object_slices, probe):
        return general(*args)
    band = object_slices.shape[2]
    width = object_slices.shape[3]
    packed = jnp.concatenate([object_slices[0], object_slices[1]], axis=-1)
    framed = jnp.concatenate(
        [shifted(packed, "scan", 1), packed, shifted(packed, "scan", -1)], axis=1
    )
    region = lax.all_gather(framed, "angle", axis=0)
    grad, probe_grad = gradients(
        region, probe, intensities, row_offsets, column_starts, slice_shifts, counts
    )
    shared = lax.psum_scatter(grad, "angle", scatter_dimension=0, tiled=False)
    total = (
        shared[:, band : 2 * band]
        + shifted(shared[:, 2 * band :], "scan", 1)
        + shifted(shared[:, :band], "scan", -1)
    )
    object_gradient = jnp.stack([total[:, :, :width], total[:, :, width:]])
    return (object_gradient, lax.psum(lax.psum(probe_grad, "scan"), "angle"))


def solution(mesh):
    return jax.shard_map(
        local,
        mesh=mesh,
        in_specs=(
            P(None, None, "scan", "angle"),
            P(),
            P("angle", "scan", None, None, None),
            P("angle", "scan", None),
            P("angle", "scan", None),
            P("angle", None),
            P("angle", "scan"),
        ),
        out_specs=(P(None, None, "scan", "angle"), P()),
        check_vma=False,
    )
```

```python
from functools import partial

import jax
import jax.numpy as jnp
import ml_dtypes
import numpy as np
from jax import lax
from jax.experimental import pallas as pl
from jax.experimental.pallas import tpu as pltpu
from jax.sharding import PartitionSpec as P


def operators(size):
    index = np.arange(size)
    turns = np.outer(index, index) % size
    fourier = np.exp(-2j * np.pi * turns / size) / np.sqrt(size)
    centred = (index + size // 2) % size - size // 2
    factor = np.exp(8j * np.pi * centred**2 / size**2)
    step = np.conj(fourier) @ (factor[:, None] * fourier)
    packed = []
    for matrix in (step, fourier):
        right = np.block([[matrix.real, matrix.imag], [-matrix.imag, matrix.real]])
        packed.append(right)
        packed.append(right.T)
    out = np.zeros((4, 2, 2 * size, 2 * size), ml_dtypes.bfloat16)
    for i, matrix in enumerate(packed):
        whole = matrix.astype(np.float32)
        high = whole.astype(ml_dtypes.bfloat16)
        out[i, 0] = high
        out[i, 1] = (whole - high.astype(np.float32)).astype(ml_dtypes.bfloat16)
    return out


def halves(x):
    high = x.astype(jnp.bfloat16)
    return high, (x - high.astype(jnp.float32)).astype(jnp.bfloat16)


def dot(a, b):
    return jnp.dot(a, b, preferred_element_type=jnp.float32)


def both_sides(waves, right, left):
    size = waves[0][0].shape[0]
    stacked = jnp.concatenate([jnp.concatenate([re, im], axis=1) for re, im in waves], axis=0)
    high, low = halves(stacked)
    out = dot(high, right[0]) + (dot(low, right[0]) + dot(high, right[1]))
    rows = [out[s * size : (s + 1) * size] for s in range(len(waves))]
    beside = jnp.concatenate(
        [
            jnp.concatenate([r[:, :size] for r in rows], axis=1),
            jnp.concatenate([r[:, size:] for r in rows], axis=1),
        ],
        axis=0,
    )
    high, low = halves(beside)
    out = dot(left[0], high) + (dot(left[0], low) + dot(left[1], high))
    return [
        (out[:size, s * size : (s + 1) * size], out[size:, s * size : (s + 1) * size])
        for s in range(len(waves))
    ]


def times(a, b):
    return (a[0] * b[0] - a[1] * b[1], a[0] * b[1] + a[1] * b[0])


def conj_times(a, b):
    return (a[0] * b[0] + a[1] * b[1], a[0] * b[1] - a[1] * b[0])


def compute_kernel(
    angles, rows_ref, cols_ref, shifts_ref, counts_ref, region_ref, probe_ref, measured_ref, mats_ref,
    grad_ref, probe_grad_ref,
):
    blocks, layers, height, lanes = region_ref.shape
    width = lanes // 2
    size = probe_ref.shape[1]
    slots = measured_ref.shape[0]
    lane = lax.broadcasted_iota(jnp.int32, (size, lanes), 1)
    lower = lane < width
    swap = lambda x: pltpu.roll(x, width, 1)
    tops = [rows_ref[s] for s in range(slots)]
    starts = [[cols_ref[s] + shifts_ref[k] for k in range(layers)] for s in range(slots)]

    def place(s, k):
        q = starts[s][k] // width
        return q, starts[s][k] - q * width

    def patch(s, k):
        q, r = place(s, k)
        rows = pl.ds(tops[s], size)
        first = region_ref[q, k, rows, :]
        second = region_ref[q + 1, k, rows, :]
        third = region_ref[jnp.minimum(q + 2, blocks - 1), k, rows, :]
        back = lax.rem(lanes - r, lanes)
        inside = lane < lanes - r
        pieces = []
        for near, far in (
            (jnp.where(lower, first, swap(second)), third),
            (jnp.where(lower, swap(first), second), swap(third)),
        ):
            pieces.append(jnp.where(inside, pltpu.roll(near, back, 1), pltpu.roll(far, back, 1)))
        return tuple(pieces)

    objects = [[patch(s, k) for k in range(layers)] for s in range(slots)]
    step_r, step_l, four_r, four_l = [(mats_ref[i, 0], mats_ref[i, 1]) for i in range(4)]
    waves = [(probe_ref[0], probe_ref[1])] * slots
    before = []
    for k in range(layers):
        before.append(waves)
        waves = [times(waves[s], objects[s][k]) for s in range(slots)]
        if k + 1 < layers:
            waves = both_sides(waves, step_r, step_l)
    far = both_sides(waves, four_r, four_l)
    grads = []
    for s in range(slots):
        weight = jnp.where(s < counts_ref[0], 2.0 / angles, 0.0)
        re, im = far[s]
        scale = weight * (re * re + im * im - measured_ref[s])
        grads.append((scale * re, scale * im))
    grads = both_sides(grads, four_l, four_r)
    grad_ref[...] = jnp.zeros(grad_ref.shape, jnp.float32)
    for k in reversed(range(layers)):
        for s in range(slots):
            re, im = conj_times(before[k][s], grads[s])
            q, r = place(s, k)
            rows = pl.ds(tops[s], size)
            re, im = pltpu.roll(re, r, 1), pltpu.roll(im, r, 1)
            zero = jnp.zeros_like(re)
            near_re, near_im = jnp.where(lane >= r, re, zero), jnp.where(lane >= r, im, zero)
            far_re, far_im = jnp.where(lane < r, re, zero), jnp.where(lane < r, im, zero)
            grad_ref[q, k, rows, :] += jnp.where(lower, near_re, swap(near_im))
            grad_ref[q + 1, k, rows, :] += jnp.where(lower, swap(near_re), near_im)
            last = jnp.minimum(q + 2, blocks - 1)
            grad_ref[last, k, rows, :] += jnp.where(lower, far_re, swap(far_im))
        grads = [conj_times(objects[s][k], grads[s]) for s in range(slots)]
        if k > 0:
            grads = both_sides(grads, step_l, step_r)
    probe_grad_ref[0] = sum(g[0] for g in grads)
    probe_grad_ref[1] = sum(g[1] for g in grads)


def gradients(region, probe, intensities, row_offsets, column_starts, slice_shifts, counts):
    angles = lax.axis_size("angle")
    smem = pl.BlockSpec(memory_space=pltpu.SMEM)
    vmem = pl.BlockSpec(memory_space=pltpu.VMEM)
    return pl.pallas_call(
        partial(compute_kernel, angles),
        out_shape=(
            jax.ShapeDtypeStruct(region.shape, jnp.float32),
            jax.ShapeDtypeStruct(probe.shape, jnp.float32),
        ),
        in_specs=[smem] * 4 + [vmem] * 4,
        out_specs=(vmem, vmem),
        compiler_params=pltpu.CompilerParams(vmem_limit_bytes=48 * 2**20),
    )(
        row_offsets.reshape(-1), column_starts.reshape(-1), slice_shifts.reshape(-1),
        counts.reshape(-1), region, probe, intensities[0, 0], jnp.asarray(operators(probe.shape[1])),
    )


MESH = pl.DeviceIdType.MESH


def flip(j, bit):
    return j + bit * (1 - 2 * lax.rem(lax.div(j, bit), 2))


def places():
    me, z = lax.axis_index("angle"), lax.axis_index("scan")
    x, y = flip(me, 2), flip(me, 4)
    return me, z, lax.rem(me, 2), (me, x, y, flip(x, 4))


def exchange(src, dst, send_sem, recv_sem, device):
    return pltpu.make_async_remote_copy(
        src_ref=src, dst_ref=dst, send_sem=send_sem, recv_sem=recv_sem, device_id=device,
        device_id_type=MESH,
    )


def gather_kernel(scans, object_ref, region_ref, stage, z_sem, plane_sem, core_sem, recv_sem):
    band, width = object_ref.shape[2:]
    me, z, core, spots = places()
    partner = flip(me, 1)
    above, below = z > 0, z < scans - 1
    for k in range(object_ref.shape[1]):
        packed = jnp.concatenate([object_ref[0, k], object_ref[1, k]], axis=1)
        stage[k] = packed
        region_ref[me, k, band : 2 * band] = packed
    barrier = pltpu.get_barrier_semaphore()

    def greet(device):
        pl.semaphore_signal(barrier, inc=1, device_id=device, device_id_type=MESH)

    for peer in (partner, spots[1], spots[2]):
        greet((peer, z))
    pl.when(above)(lambda: greet((me, z - 1)))
    pl.when(below)(lambda: greet((me, z + 1)))
    zeros = jnp.zeros(region_ref.shape[:2] + (band,) + region_ref.shape[3:], jnp.float32)

    @pl.when(jnp.logical_not(above))
    def _():
        region_ref[:, :, :band] = zeros

    @pl.when(jnp.logical_not(below))
    def _():
        region_ref[:, :, 2 * band :] = zeros

    pl.semaphore_wait(barrier, 3 + above.astype(jnp.int32) + below.astype(jnp.int32))

    def piece(j, part):
        return region_ref.at[j, :, pl.ds(part * band, band), :]

    def to(src, j, part, sem, device):
        return exchange(src, piece(j, part), sem, recv_sem.at[part, j], device)

    def arrive(j, part):
        to(piece(j, part), j, part, core_sem.at[0, 0], (partner, z)).wait_recv()

    pending = []

    def upright(i, src):
        up = to(src, spots[i], 2, z_sem.at[0, i], (me, z - 1))
        down = to(src, spots[i], 0, z_sem.at[1, i], (me, z + 1))
        pl.when(above)(lambda: up.start())
        pl.when(below)(lambda: down.start())
        pending.append((above, up))
        pending.append((below, down))

    def share(i, part, src):
        copy = to(src, spots[i], part, core_sem.at[part, i], (partner, z))
        copy.start()
        pending.append((None, copy))

    def across(src, j, n, device):
        copy = to(src, j, 1, plane_sem.at[n], (device, z))
        copy.start()
        pending.append((None, copy))

    across(stage, me, 0, spots[1])
    across(stage, me, 1, spots[2])
    upright(0, stage)
    share(0, 1, stage)
    arrive(spots[1], 1)
    upright(1, piece(spots[1], 1))
    arrive(spots[2], 1)
    source = spots[1] + core * (spots[2] - spots[1])
    target = spots[2] + core * (spots[1] - spots[2])
    across(piece(source, 1), source, 2, target)
    upright(2, piece(spots[2], 1))
    share(1, 1, piece(spots[1], 1))
    share(2, 1, piece(spots[2], 1))
    arrive(spots[3], 1)
    upright(3, piece(spots[3], 1))
    share(3, 1, piece(spots[3], 1))
    for i in range(4):
        for part, when in ((0, above), (2, below)):

            copy = to(piece(spots[i], part), spots[i], part, core_sem.at[part, i], (partner, z))
            pending.append((when, copy))

            @pl.when(when)
            def _(i=i, part=part, copy=copy):
                arrive(spots[i], part)
                copy.start()

    for part, when in ((1, None), (0, above), (2, below)):
        for i in range(4):
            wait = partial(arrive, spots[i] + 1 - 2 * core, part)
            wait() if when is None else pl.when(when)(wait)
    for when, copy in pending:
        copy.wait_send() if when is None else pl.when(when)(lambda copy=copy: copy.wait_send())


def reduce_kernel(
    scans, grad_ref, probe_ref, object_ref, total_ref,
    core_in, held, z_in, ready, plane_in, last_in, passed, probe_in, scan_in, mine,
    core_sem, z_sem, plane_sem, angle_sem, scan_sem, all_sem,
):
    angles, layers, height, lanes = grad_ref.shape
    band = height // 3
    rows = probe_ref.shape[0] // angles
    me, z, core, spots = places()
    partner = flip(me, 1)
    above, below = z > 0, z < scans - 1
    barrier = pltpu.get_barrier_semaphore()
    peers = [lax.rem(me + d, angles) for d in range(1, angles)]
    levels = [lax.rem(z + d, scans) for d in range(1, scans)]
    for device in [(peer, z) for peer in peers] + [(me, level) for level in levels]:
        pl.semaphore_signal(barrier, inc=1, device_id=device, device_id_type=MESH)
    pl.semaphore_wait(barrier, angles + scans - 2)
    pending = []

    def go(src, dst, send_sem, recv_sem, device):
        copy = exchange(src, dst, send_sem, recv_sem, device)
        copy.start()
        pending.append((None, copy))

    def arrive(dst, recv_sem):
        exchange(dst, dst, core_sem.at[0, 0], recv_sem, (partner, z)).wait_recv()

    order = (3, 1, 2, 0)
    for i in order:
        go(grad_ref.at[spots[i] + 1 - 2 * core], core_in.at[i], core_sem.at[0, i], core_sem.at[1, i], (partner, z))
    for d, peer in enumerate(peers):
        go(
            probe_ref.at[pl.ds(peer * rows, rows)], probe_in.at[me],
            angle_sem.at[0, d], angle_sem.at[1, me], (peer, z),
        )
    for i in order:
        arrive(core_in.at[i], core_sem.at[1, i])
        for part in (0, 2, 1):
            span = pl.ds(part * band, band)
            held[i, :, span] = grad_ref[spots[i], :, span] + core_in[i, :, span]
        up = exchange(
            held.at[i, :, pl.ds(0, band)], z_in.at[1, i], z_sem.at[0, 0, i], z_sem.at[1, 1, i], (me, z - 1)
        )
        down = exchange(
            held.at[i, :, pl.ds(2 * band, band)], z_in.at[0, i], z_sem.at[0, 1, i], z_sem.at[1, 0, i], (me, z + 1)
        )
        pl.when(above)(lambda up=up: up.start())
        pl.when(below)(lambda down=down: down.start())
        pending.append((above, up))
        pending.append((below, down))
    for peer in peers:
        arrive(probe_in.at[peer], angle_sem.at[1, peer])
    probe_in[me] = probe_ref[pl.ds(me * rows, rows)]
    part_sum = probe_in[0]
    for j in range(1, angles):
        part_sum += probe_in[j]
    passed[...] = part_sum
    scan_in[z] = part_sum
    for d, level in enumerate(levels):
        go(passed, scan_in.at[z], scan_sem.at[0, d], scan_sem.at[1, z], (me, level))
    first, second = 2 - core, 1 + core
    near = spots[2] + core * (spots[1] - spots[2])
    other = spots[1] + core * (spots[2] - spots[1])
    for i in order:
        ready[i] = held[i, :, pl.ds(band, band)]

        @pl.when(above)
        def _():
            arrive(z_in.at[0, i], z_sem.at[1, 0, i])
            ready[i] += z_in[0, i]

        @pl.when(below)
        def _():
            arrive(z_in.at[1, i], z_sem.at[1, 1, i])
            ready[i] += z_in[1, i]

        if i == 3:
            go(ready.at[3], plane_in.at[1], plane_sem.at[0, 1], plane_sem.at[1, 1], (near, z))
        if i == 2:
            go(ready.at[first], plane_in.at[0], plane_sem.at[0, 0], plane_sem.at[1, 0], (near, z))
    arrive(plane_in.at[1], plane_sem.at[1, 1])
    mine[...] = ready[second] + plane_in[1]
    go(mine, last_in, plane_sem.at[0, 2], plane_sem.at[1, 2], (other, z))
    for level in levels:
        arrive(scan_in.at[level], scan_sem.at[1, level])
    whole = scan_in[0]
    for j in range(1, scans):
        whole += scan_in[j]
    own = pl.ds(me * rows, rows)
    total_ref[own] = whole
    passed_all = total_ref.at[own]
    for d, peer in enumerate(peers):
        go(passed_all, total_ref.at[own], all_sem.at[0, d], all_sem.at[1, me], (peer, z))
    arrive(plane_in.at[0], plane_sem.at[1, 0])
    arrive(last_in, plane_sem.at[1, 2])
    result = ready[0] + plane_in[0] + last_in[...]
    object_ref[0] = result[:, :, : lanes // 2]
    object_ref[1] = result[:, :, lanes // 2 :]
    for peer in peers:
        arrive(total_ref.at[pl.ds(peer * rows, rows)], all_sem.at[1, peer])
    for when, copy in pending:
        copy.wait_send() if when is None else pl.when(when)(lambda copy=copy: copy.wait_send())


def gather(object_slices):
    angles, scans = lax.axis_size("angle"), lax.axis_size("scan")
    parts, layers, band, width = object_slices.shape
    vmem = pl.BlockSpec(memory_space=pltpu.VMEM)
    dma = pltpu.SemaphoreType.DMA
    return pl.pallas_call(
        partial(gather_kernel, scans),
        out_shape=jax.ShapeDtypeStruct((angles, layers, 3 * band, 2 * width), jnp.float32),
        in_specs=[vmem],
        out_specs=vmem,
        scratch_shapes=[
            pltpu.VMEM((layers, band, 2 * width), jnp.float32),
            dma((2, 4)), dma((3,)), dma((3, 4)), dma((3, angles)),
        ],
        compiler_params=pltpu.CompilerParams(
            collective_id=0, has_side_effects=True, vmem_limit_bytes=32 * 2**20
        ),
    )(object_slices)


def reduce(grad, probe_grad):
    angles, scans = lax.axis_size("angle"), lax.axis_size("scan")
    layers, height, lanes = grad.shape[1:]
    band = height // 3
    flat = probe_grad.reshape(-1, probe_grad.shape[-1])
    rows = flat.shape[0] // angles
    block = (layers, band, lanes)
    small = (rows, flat.shape[1])
    vmem = pl.BlockSpec(memory_space=pltpu.VMEM)
    dma = pltpu.SemaphoreType.DMA
    buffer = lambda *shape: pltpu.VMEM(shape, jnp.float32)
    object_grad, total = pl.pallas_call(
        partial(reduce_kernel, scans),
        out_shape=(
            jax.ShapeDtypeStruct((2, layers, band, lanes // 2), jnp.float32),
            jax.ShapeDtypeStruct(flat.shape, jnp.float32),
        ),
        in_specs=[vmem, vmem],
        out_specs=(vmem, vmem),
        scratch_shapes=[
            buffer(4, layers, height, lanes), buffer(4, layers, height, lanes), buffer(2, 4, *block),
            buffer(4, *block), buffer(2, *block), buffer(*block), buffer(*small),
            buffer(angles, *small), buffer(scans, *small), buffer(*block),
            dma((2, 4)), dma((2, 2, 4)), dma((2, 3)), dma((2, angles)), dma((2, scans)),
            dma((2, angles)),
        ],
        compiler_params=pltpu.CompilerParams(
            collective_id=1, has_side_effects=True, vmem_limit_bytes=32 * 2**20
        ),
    )(grad, flat)
    return object_grad, total.reshape(probe_grad.shape)


def padded(cells, sides, width):
    for axis, dim in sides:
        count = lax.axis_size(axis)
        ends = count - 1
        head = lax.slice_in_dim(cells, 0, width, axis=dim)
        tail = lax.slice_in_dim(cells, cells.shape[dim] - width, cells.shape[dim], axis=dim)
        cells = jnp.concatenate(
            [
                lax.ppermute(tail, axis, [(i, (i + 1) % count) for i in range(ends)]),
                cells,
                lax.ppermute(head, axis, [((i + 1) % count, i) for i in range(ends)]),
            ],
            axis=dim,
        )
    return cells


def propagator(size):
    index = jnp.arange(size, dtype=jnp.int32)
    centred = ((index + size // 2) % size - size // 2).astype(jnp.float32)
    radius = centred[:, None] * centred[:, None] + centred[None, :] * centred[None, :]
    phase = 8.0 * jnp.pi * radius / (size * size)
    return (jnp.cos(phase), jnp.sin(phase))


def tables(size):
    index = jnp.arange(size, dtype=jnp.int32)
    turns = index[:, None] * index[None, :] % size
    phase = 2.0 * jnp.pi * turns.astype(jnp.float32) / size
    scale = 1.0 / jnp.sqrt(jnp.float32(size))
    return (jnp.cos(phase) * scale, jnp.sin(phase) * scale)


def matmul(first, second):
    return jnp.dot(
        first, second, precision=lax.Precision.HIGHEST, preferred_element_type=jnp.float32
    )


def transform(real_part, imag_part, cosine, sine, sign):
    left_re = matmul(cosine, real_part) - sign * matmul(sine, imag_part)
    left_im = matmul(cosine, imag_part) + sign * matmul(sine, real_part)
    right_re = matmul(left_re, cosine) - sign * matmul(left_im, sine)
    right_im = matmul(left_im, cosine) + sign * matmul(left_re, sine)
    return (right_re, right_im)


def local_loss(slab, probe, measured, weight, cosine, sine, kern_re, kern_im):
    wave_re, wave_im = (probe[0], probe[1])
    layers = slab.shape[1]
    for k in range(layers):
        object_re, object_im = (slab[0, k], slab[1, k])
        wave_re, wave_im = (
            wave_re * object_re - wave_im * object_im,
            wave_re * object_im + wave_im * object_re,
        )
        if k + 1 < layers:
            freq_re, freq_im = transform(wave_re, wave_im, cosine, sine, -1.0)
            freq_re, freq_im = (
                freq_re * kern_re - freq_im * kern_im,
                freq_re * kern_im + freq_im * kern_re,
            )
            wave_re, wave_im = transform(freq_re, freq_im, cosine, sine, 1.0)
    far_re, far_im = transform(wave_re, wave_im, cosine, sine, -1.0)
    differ = far_re * far_re + far_im * far_im - measured
    return weight * jnp.sum(differ * differ)


def general(object_slices, probe, intensities, row_offsets, column_starts, slice_shifts, counts):
    band = object_slices.shape[2]
    framed = padded(object_slices, (("scan", 2),), band)
    region = lax.all_gather(framed, "angle", axis=3, tiled=True)
    size = probe.shape[1]
    slots = row_offsets.shape[2]
    layers = region.shape[1]
    angles = lax.axis_size("angle")
    cosine, sine = tables(size)
    kern_re, kern_im = propagator(size)
    shifts = slice_shifts[0]
    zero = jnp.zeros((), jnp.int32)

    def visit(slot, carry):
        gradient_region, gradient_probe = carry
        top = row_offsets[0, 0, slot]
        start = column_starts[0, 0, slot]
        slab = jnp.concatenate(
            [
                lax.dynamic_slice(
                    region, (zero, zero + k, top, start + shifts[k]), (2, 1, size, size)
                )
                for k in range(layers)
            ],
            axis=1,
        )
        weight = jnp.where(slot < counts[0, 0], 0.5 / angles, 0.0).astype(jnp.float32)
        measured = intensities[0, 0, slot]
        scorer = partial(
            local_loss,
            measured=measured,
            weight=weight,
            cosine=cosine,
            sine=sine,
            kern_re=kern_re,
            kern_im=kern_im,
        )
        loss, pull = jax.vjp(scorer, slab, probe)
        slab_grad, probe_grad = pull(jnp.ones_like(loss))
        for k in range(layers):
            place = (zero, zero + k, top, start + shifts[k])
            current = lax.dynamic_slice(gradient_region, place, (2, 1, size, size))
            gradient_region = lax.dynamic_update_slice(
                gradient_region, current + slab_grad[:, k : k + 1], place
            )
        return (gradient_region, gradient_probe + probe_grad)

    start_carry = (jnp.zeros(region.shape, jnp.float32), jnp.zeros(probe.shape, jnp.float32))
    gradient_region, gradient_probe = lax.fori_loop(0, slots, visit, start_carry)
    shared = lax.psum_scatter(gradient_region, "angle", scatter_dimension=3, tiled=True)
    edges = jnp.concatenate([shared[:, :, :band], shared[:, :, 2 * band :]], axis=2)
    rimmed = padded(edges, (("scan", 2),), band)
    object_gradient = shared[:, :, band : 2 * band] + rimmed[:, :, :band] + rimmed[:, :, 3 * band :]
    group_total = lax.psum(gradient_probe, "scan")
    probe_gradient = lax.psum(group_total, "angle")
    return (object_gradient, probe_gradient)


def packable(object_slices, probe):
    size = probe.shape[1]
    band, width = object_slices.shape[2:]
    return 2 * width == size == 128 and band % 8 == 0 and lax.axis_size("angle") == 2**3


def local(object_slices, probe, intensities, row_offsets, column_starts, slice_shifts, counts):
    args = (object_slices, probe, intensities, row_offsets, column_starts, slice_shifts, counts)
    if not packable(object_slices, probe):
        return general(*args)
    region = gather(object_slices)
    grad, probe_grad = gradients(
        region, probe, intensities, row_offsets, column_starts, slice_shifts, counts
    )
    return reduce(grad, probe_grad)


def solution(mesh):
    return jax.shard_map(
        local,
        mesh=mesh,
        in_specs=(
            P(None, None, "scan", "angle"),
            P(),
            P("angle", "scan", None, None, None),
            P("angle", "scan", None),
            P("angle", "scan", None),
            P("angle", None),
            P("angle", "scan"),
        ),
        out_specs=(P(None, None, "scan", "angle"), P()),
        check_vma=False,
    )
```

```python
from functools import partial

import jax
import jax.numpy as jnp
import ml_dtypes
import numpy as np
from jax import lax
from jax.experimental import pallas as pl
from jax.experimental.pallas import tpu as pltpu
from jax.sharding import PartitionSpec as P


def operators(size):
    index = np.arange(size)
    turns = np.outer(index, index) % size
    fourier = np.exp(-2j * np.pi * turns / size) / np.sqrt(size)
    centred = (index + size // 2) % size - size // 2
    factor = np.exp(8j * np.pi * centred**2 / size**2)
    step = np.conj(fourier) @ (factor[:, None] * fourier)
    packed = []
    for matrix in (step, fourier):
        right = np.block([[matrix.real, matrix.imag], [-matrix.imag, matrix.real]])
        packed.append(right)
        packed.append(right.T)
    out = np.zeros((4, 2, 2 * size, 2 * size), ml_dtypes.bfloat16)
    for i, matrix in enumerate(packed):
        whole = matrix.astype(np.float32)
        high = whole.astype(ml_dtypes.bfloat16)
        out[i, 0] = high
        out[i, 1] = (whole - high.astype(np.float32)).astype(ml_dtypes.bfloat16)
    return out


def halves(x):
    high = x.astype(jnp.bfloat16)
    return high, (x - high.astype(jnp.float32)).astype(jnp.bfloat16)


def dot(a, b):
    return jnp.dot(a, b, preferred_element_type=jnp.float32)


def both_sides(waves, right, left):
    size = waves[0][0].shape[0]
    stacked = jnp.concatenate([jnp.concatenate([re, im], axis=1) for re, im in waves], axis=0)
    high, low = halves(stacked)
    out = dot(high, right[0]) + (dot(low, right[0]) + dot(high, right[1]))
    rows = [out[s * size : (s + 1) * size] for s in range(len(waves))]
    beside = jnp.concatenate(
        [
            jnp.concatenate([r[:, :size] for r in rows], axis=1),
            jnp.concatenate([r[:, size:] for r in rows], axis=1),
        ],
        axis=0,
    )
    high, low = halves(beside)
    out = dot(left[0], high) + (dot(left[0], low) + dot(left[1], high))
    return [
        (out[:size, s * size : (s + 1) * size], out[size:, s * size : (s + 1) * size])
        for s in range(len(waves))
    ]


def times(a, b):
    return (a[0] * b[0] - a[1] * b[1], a[0] * b[1] + a[1] * b[0])


def conj_times(a, b):
    return (a[0] * b[0] + a[1] * b[1], a[0] * b[1] - a[1] * b[0])


def compute_kernel(
    angles, rows_ref, cols_ref, shifts_ref, counts_ref, region_ref, probe_ref, measured_ref, mats_ref,
    grad_ref, probe_grad_ref,
):
    blocks, layers, height, lanes = region_ref.shape
    width = lanes // 2
    size = probe_ref.shape[1]
    slots = measured_ref.shape[0]
    lane = lax.broadcasted_iota(jnp.int32, (size, lanes), 1)
    lower = lane < width
    swap = lambda x: pltpu.roll(x, width, 1)
    tops = [rows_ref[s] for s in range(slots)]
    starts = [[cols_ref[s] + shifts_ref[k] for k in range(layers)] for s in range(slots)]

    def place(s, k):
        q = starts[s][k] // width
        return q, starts[s][k] - q * width

    def patch(s, k):
        q, r = place(s, k)
        rows = pl.ds(tops[s], size)
        first = region_ref[q, k, rows, :]
        second = region_ref[q + 1, k, rows, :]
        third = region_ref[jnp.minimum(q + 2, blocks - 1), k, rows, :]
        back = lax.rem(lanes - r, lanes)
        inside = lane < lanes - r
        pieces = []
        for near, far in (
            (jnp.where(lower, first, swap(second)), third),
            (jnp.where(lower, swap(first), second), swap(third)),
        ):
            pieces.append(jnp.where(inside, pltpu.roll(near, back, 1), pltpu.roll(far, back, 1)))
        return tuple(pieces)

    objects = [[patch(s, k) for k in range(layers)] for s in range(slots)]
    step_r, step_l, four_r, four_l = [(mats_ref[i, 0], mats_ref[i, 1]) for i in range(4)]
    waves = [(probe_ref[0], probe_ref[1])] * slots
    before = []
    for k in range(layers):
        before.append(waves)
        waves = [times(waves[s], objects[s][k]) for s in range(slots)]
        if k + 1 < layers:
            waves = both_sides(waves, step_r, step_l)
    far = both_sides(waves, four_r, four_l)
    grads = []
    for s in range(slots):
        weight = jnp.where(s < counts_ref[0], 2.0 / angles, 0.0)
        re, im = far[s]
        scale = weight * (re * re + im * im - measured_ref[s])
        grads.append((scale * re, scale * im))
    grads = both_sides(grads, four_l, four_r)
    grad_ref[...] = jnp.zeros(grad_ref.shape, jnp.float32)
    for k in reversed(range(layers)):
        for s in range(slots):
            re, im = conj_times(before[k][s], grads[s])
            q, r = place(s, k)
            rows = pl.ds(tops[s], size)
            re, im = pltpu.roll(re, r, 1), pltpu.roll(im, r, 1)
            zero = jnp.zeros_like(re)
            near_re, near_im = jnp.where(lane >= r, re, zero), jnp.where(lane >= r, im, zero)
            far_re, far_im = jnp.where(lane < r, re, zero), jnp.where(lane < r, im, zero)
            grad_ref[q, k, rows, :] += jnp.where(lower, near_re, swap(near_im))
            grad_ref[q + 1, k, rows, :] += jnp.where(lower, swap(near_re), near_im)
            last = jnp.minimum(q + 2, blocks - 1)
            grad_ref[last, k, rows, :] += jnp.where(lower, far_re, swap(far_im))
        grads = [conj_times(objects[s][k], grads[s]) for s in range(slots)]
        if k > 0:
            grads = both_sides(grads, step_l, step_r)
    probe_grad_ref[0] = sum(g[0] for g in grads)
    probe_grad_ref[1] = sum(g[1] for g in grads)


def gradients(region, probe, intensities, row_offsets, column_starts, slice_shifts, counts):
    angles = lax.axis_size("angle")
    smem = pl.BlockSpec(memory_space=pltpu.SMEM)
    vmem = pl.BlockSpec(memory_space=pltpu.VMEM)
    return pl.pallas_call(
        partial(compute_kernel, angles),
        out_shape=(
            jax.ShapeDtypeStruct(region.shape, jnp.float32),
            jax.ShapeDtypeStruct(probe.shape, jnp.float32),
        ),
        in_specs=[smem] * 4 + [vmem] * 4,
        out_specs=(vmem, vmem),
        compiler_params=pltpu.CompilerParams(vmem_limit_bytes=48 * 2**20),
    )(
        row_offsets.reshape(-1), column_starts.reshape(-1), slice_shifts.reshape(-1),
        counts.reshape(-1), region, probe, intensities[0, 0], jnp.asarray(operators(probe.shape[1])),
    )


MESH = pl.DeviceIdType.MESH


def flip(j, bit):
    return j + bit * (1 - 2 * lax.rem(lax.div(j, bit), 2))


def places():
    me, z = lax.axis_index("angle"), lax.axis_index("scan")
    x, y = flip(me, 2), flip(me, 4)
    return me, z, lax.rem(me, 2), (me, x, y, flip(x, 4))


def exchange(src, dst, send_sem, recv_sem, device):
    return pltpu.make_async_remote_copy(
        src_ref=src, dst_ref=dst, send_sem=send_sem, recv_sem=recv_sem, device_id=device,
        device_id_type=MESH,
    )


def gather_kernel(scans, object_ref, region_ref, stage, z_sem, plane_sem, core_sem, recv_sem):
    band, width = object_ref.shape[2:]
    me, z, core, spots = places()
    partner = flip(me, 1)
    above, below = z > 0, z < scans - 1
    for k in range(object_ref.shape[1]):
        packed = jnp.concatenate([object_ref[0, k], object_ref[1, k]], axis=1)
        stage[k] = packed
        region_ref[me, k, band : 2 * band] = packed
    barrier = pltpu.get_barrier_semaphore()

    def greet(device):
        pl.semaphore_signal(barrier, inc=1, device_id=device, device_id_type=MESH)

    for peer in (partner, spots[1], spots[2]):
        greet((peer, z))
    pl.when(above)(lambda: greet((me, z - 1)))
    pl.when(below)(lambda: greet((me, z + 1)))
    zeros = jnp.zeros(region_ref.shape[:2] + (band,) + region_ref.shape[3:], jnp.float32)

    @pl.when(jnp.logical_not(above))
    def _():
        region_ref[:, :, :band] = zeros

    @pl.when(jnp.logical_not(below))
    def _():
        region_ref[:, :, 2 * band :] = zeros

    pl.semaphore_wait(barrier, 3 + above.astype(jnp.int32) + below.astype(jnp.int32))

    def piece(j, part):
        return region_ref.at[j, :, pl.ds(part * band, band), :]

    def to(src, j, part, sem, device):
        return exchange(src, piece(j, part), sem, recv_sem.at[part, j], device)

    def arrive(j, part):
        to(piece(j, part), j, part, core_sem.at[0, 0], (partner, z)).wait_recv()

    pending = []

    def upright(i, j, src):
        up = to(src, j, 2, z_sem.at[0, i], (me, z - 1))
        down = to(src, j, 0, z_sem.at[1, i], (me, z + 1))
        pl.when(above)(lambda: up.start())
        pl.when(below)(lambda: down.start())
        pending.append((above, up))
        pending.append((below, down))

    def share(i, part, src):
        copy = to(src, spots[i], part, core_sem.at[part, i], (partner, z))
        copy.start()
        pending.append((None, copy))

    def across(src, j, n, device):
        copy = to(src, j, 1, plane_sem.at[n], (device, z))
        copy.start()
        pending.append((None, copy))

    source = spots[1] + core * (spots[2] - spots[1])
    target = spots[2] + core * (spots[1] - spots[2])
    upright(0, me, stage)
    across(stage, me, 0, spots[1])
    across(stage, me, 1, spots[2])
    share(0, 1, stage)
    arrive(source, 1)
    across(piece(source, 1), source, 2, target)
    arrive(target, 1)
    upright(1, target, piece(target, 1))
    share(1, 1, piece(spots[1], 1))
    share(2, 1, piece(spots[2], 1))

    def relay(i, j, part, when, onward=None):
        copies = [to(piece(j, part), j, part, core_sem.at[part, i], (partner, z))]
        if onward is not None:
            copies.insert(0, to(piece(j, part), j, part, plane_sem.at[onward], (source, z)))
        pending.extend((when, copy) for copy in copies)

        @pl.when(when)
        def _():
            arrive(j, part)
            for copy in copies:
                copy.start()

    relay(0, me, 0, above, 3)
    relay(0, me, 2, below, 4)
    arrive(spots[3], 1)
    upright(2, spots[3], piece(spots[3], 1))
    share(3, 1, piece(spots[3], 1))
    for i, j in ((2 - core, target), (1 + core, source), (3, spots[3])):
        relay(i, j, 0, above)
        relay(i, j, 2, below)
    for part, when in ((1, None), (0, above), (2, below)):
        for i in range(4):
            wait = partial(arrive, spots[i] + 1 - 2 * core, part)
            wait() if when is None else pl.when(when)(wait)
    for when, copy in pending:
        copy.wait_send() if when is None else pl.when(when)(lambda copy=copy: copy.wait_send())


def reduce_kernel(
    scans, grad_ref, probe_ref, object_ref, total_ref,
    core_in, held, z_in, ready, plane_in, last_in, side_in, passed, probe_in, scan_in, mine,
    core_sem, z_sem, plane_sem, side_sem, angle_sem, scan_sem, all_sem,
):
    angles, layers, height, lanes = grad_ref.shape
    band = height // 3
    rows = probe_ref.shape[0] // angles
    me, z, core, spots = places()
    partner = flip(me, 1)
    above, below = z > 0, z < scans - 1
    barrier = pltpu.get_barrier_semaphore()
    peers = [lax.rem(me + d, angles) for d in range(1, angles)]
    levels = [lax.rem(z + d, scans) for d in range(1, scans)]
    for device in [(peer, z) for peer in peers] + [(me, level) for level in levels]:
        pl.semaphore_signal(barrier, inc=1, device_id=device, device_id_type=MESH)
    pl.semaphore_wait(barrier, angles + scans - 2)
    pending = []

    def go(src, dst, send_sem, recv_sem, device):
        copy = exchange(src, dst, send_sem, recv_sem, device)
        copy.start()
        pending.append((None, copy))

    def arrive(dst, recv_sem):
        exchange(dst, dst, core_sem.at[0, 0], recv_sem, (partner, z)).wait_recv()

    first, second = 2 - core, 1 + core
    near = spots[2] + core * (spots[1] - spots[2])
    other = spots[1] + core * (spots[2] - spots[1])
    for i, j in ((1 + core, other), (3, spots[3]), (2 - core, near), (0, me)):
        go(grad_ref.at[j + 1 - 2 * core], core_in.at[i], core_sem.at[0, i], core_sem.at[1, i], (partner, z))
    for d, peer in enumerate(peers):
        go(
            probe_ref.at[pl.ds(peer * rows, rows)], probe_in.at[me],
            angle_sem.at[0, d], angle_sem.at[1, me], (peer, z),
        )
    ends = (pl.ds(0, band), pl.ds(2 * band, band))

    def upright(i):
        up = exchange(
            held.at[i, :, ends[0]], z_in.at[1, i], z_sem.at[0, 0, i], z_sem.at[1, 1, i], (me, z - 1)
        )
        down = exchange(
            held.at[i, :, ends[1]], z_in.at[0, i], z_sem.at[0, 1, i], z_sem.at[1, 0, i], (me, z + 1)
        )
        pl.when(above)(lambda: up.start())
        pl.when(below)(lambda: down.start())
        pending.append((above, up))
        pending.append((below, down))

    for i, j in ((second, other), (3, spots[3]), (first, near), (0, me)):
        arrive(core_in.at[i], core_sem.at[1, i])
        for part in (0, 2, 1):
            span = pl.ds(part * band, band)
            held[i, :, span] = grad_ref[j, :, span] + core_in[i, :, span]
        if i is second:
            for n in range(2):
                go(held.at[second, :, ends[n]], side_in.at[n], side_sem.at[0, n], side_sem.at[1, n], (other, z))
        elif j is not me:
            upright(i)
    for n in range(2):
        arrive(side_in.at[n], side_sem.at[1, n])
        held[0, :, ends[n]] += side_in[n]
    upright(0)
    for peer in peers:
        arrive(probe_in.at[peer], angle_sem.at[1, peer])
    probe_in[me] = probe_ref[pl.ds(me * rows, rows)]
    part_sum = probe_in[0]
    for j in range(1, angles):
        part_sum += probe_in[j]
    passed[...] = part_sum
    scan_in[z] = part_sum
    for d, level in enumerate(levels):
        go(passed, scan_in.at[z], scan_sem.at[0, d], scan_sem.at[1, z], (me, level))
    middle = pl.ds(band, band)
    ready[second] = held[second, :, middle]

    def collect(i):
        ready[i] = held[i, :, middle]

        @pl.when(above)
        def _():
            arrive(z_in.at[0, i], z_sem.at[1, 0, i])
            ready[i] += z_in[0, i]

        @pl.when(below)
        def _():
            arrive(z_in.at[1, i], z_sem.at[1, 1, i])
            ready[i] += z_in[1, i]

    collect(3)
    go(ready.at[3], plane_in.at[1], plane_sem.at[0, 1], plane_sem.at[1, 1], (near, z))
    collect(first)
    go(ready.at[first], plane_in.at[0], plane_sem.at[0, 0], plane_sem.at[1, 0], (near, z))
    arrive(plane_in.at[1], plane_sem.at[1, 1])
    mine[...] = ready[second] + plane_in[1]
    go(mine, last_in, plane_sem.at[0, 2], plane_sem.at[1, 2], (other, z))
    for level in levels:
        arrive(scan_in.at[level], scan_sem.at[1, level])
    whole = scan_in[0]
    for j in range(1, scans):
        whole += scan_in[j]
    own = pl.ds(me * rows, rows)
    total_ref[own] = whole
    passed_all = total_ref.at[own]
    for d, peer in enumerate(peers):
        go(passed_all, total_ref.at[own], all_sem.at[0, d], all_sem.at[1, me], (peer, z))
    collect(0)
    arrive(plane_in.at[0], plane_sem.at[1, 0])
    arrive(last_in, plane_sem.at[1, 2])
    result = ready[0] + plane_in[0] + last_in[...]
    object_ref[0] = result[:, :, : lanes // 2]
    object_ref[1] = result[:, :, lanes // 2 :]
    for peer in peers:
        arrive(total_ref.at[pl.ds(peer * rows, rows)], all_sem.at[1, peer])
    for when, copy in pending:
        copy.wait_send() if when is None else pl.when(when)(lambda copy=copy: copy.wait_send())


def gather(object_slices):
    angles, scans = lax.axis_size("angle"), lax.axis_size("scan")
    parts, layers, band, width = object_slices.shape
    vmem = pl.BlockSpec(memory_space=pltpu.VMEM)
    dma = pltpu.SemaphoreType.DMA
    return pl.pallas_call(
        partial(gather_kernel, scans),
        out_shape=jax.ShapeDtypeStruct((angles, layers, 3 * band, 2 * width), jnp.float32),
        in_specs=[vmem],
        out_specs=vmem,
        scratch_shapes=[
            pltpu.VMEM((layers, band, 2 * width), jnp.float32),
            dma((2, 3)), dma((5,)), dma((3, 4)), dma((3, angles)),
        ],
        compiler_params=pltpu.CompilerParams(
            collective_id=0, has_side_effects=True, vmem_limit_bytes=32 * 2**20
        ),
    )(object_slices)


def reduce(grad, probe_grad):
    angles, scans = lax.axis_size("angle"), lax.axis_size("scan")
    layers, height, lanes = grad.shape[1:]
    band = height // 3
    flat = probe_grad.reshape(-1, probe_grad.shape[-1])
    rows = flat.shape[0] // angles
    block = (layers, band, lanes)
    small = (rows, flat.shape[1])
    vmem = pl.BlockSpec(memory_space=pltpu.VMEM)
    dma = pltpu.SemaphoreType.DMA
    buffer = lambda *shape: pltpu.VMEM(shape, jnp.float32)
    object_grad, total = pl.pallas_call(
        partial(reduce_kernel, scans),
        out_shape=(
            jax.ShapeDtypeStruct((2, layers, band, lanes // 2), jnp.float32),
            jax.ShapeDtypeStruct(flat.shape, jnp.float32),
        ),
        in_specs=[vmem, vmem],
        out_specs=(vmem, vmem),
        scratch_shapes=[
            buffer(4, layers, height, lanes), buffer(4, layers, height, lanes), buffer(2, 4, *block),
            buffer(4, *block), buffer(2, *block), buffer(*block), buffer(2, *block), buffer(*small),
            buffer(angles, *small), buffer(scans, *small), buffer(*block),
            dma((2, 4)), dma((2, 2, 4)), dma((2, 3)), dma((2, 2)), dma((2, angles)), dma((2, scans)),
            dma((2, angles)),
        ],
        compiler_params=pltpu.CompilerParams(
            collective_id=1, has_side_effects=True, vmem_limit_bytes=32 * 2**20
        ),
    )(grad, flat)
    return object_grad, total.reshape(probe_grad.shape)


def padded(cells, sides, width):
    for axis, dim in sides:
        count = lax.axis_size(axis)
        ends = count - 1
        head = lax.slice_in_dim(cells, 0, width, axis=dim)
        tail = lax.slice_in_dim(cells, cells.shape[dim] - width, cells.shape[dim], axis=dim)
        cells = jnp.concatenate(
            [
                lax.ppermute(tail, axis, [(i, (i + 1) % count) for i in range(ends)]),
                cells,
                lax.ppermute(head, axis, [((i + 1) % count, i) for i in range(ends)]),
            ],
            axis=dim,
        )
    return cells


def propagator(size):
    index = jnp.arange(size, dtype=jnp.int32)
    centred = ((index + size // 2) % size - size // 2).astype(jnp.float32)
    radius = centred[:, None] * centred[:, None] + centred[None, :] * centred[None, :]
    phase = 8.0 * jnp.pi * radius / (size * size)
    return (jnp.cos(phase), jnp.sin(phase))


def tables(size):
    index = jnp.arange(size, dtype=jnp.int32)
    turns = index[:, None] * index[None, :] % size
    phase = 2.0 * jnp.pi * turns.astype(jnp.float32) / size
    scale = 1.0 / jnp.sqrt(jnp.float32(size))
    return (jnp.cos(phase) * scale, jnp.sin(phase) * scale)


def matmul(first, second):
    return jnp.dot(
        first, second, precision=lax.Precision.HIGHEST, preferred_element_type=jnp.float32
    )


def transform(real_part, imag_part, cosine, sine, sign):
    left_re = matmul(cosine, real_part) - sign * matmul(sine, imag_part)
    left_im = matmul(cosine, imag_part) + sign * matmul(sine, real_part)
    right_re = matmul(left_re, cosine) - sign * matmul(left_im, sine)
    right_im = matmul(left_im, cosine) + sign * matmul(left_re, sine)
    return (right_re, right_im)


def local_loss(slab, probe, measured, weight, cosine, sine, kern_re, kern_im):
    wave_re, wave_im = (probe[0], probe[1])
    layers = slab.shape[1]
    for k in range(layers):
        object_re, object_im = (slab[0, k], slab[1, k])
        wave_re, wave_im = (
            wave_re * object_re - wave_im * object_im,
            wave_re * object_im + wave_im * object_re,
        )
        if k + 1 < layers:
            freq_re, freq_im = transform(wave_re, wave_im, cosine, sine, -1.0)
            freq_re, freq_im = (
                freq_re * kern_re - freq_im * kern_im,
                freq_re * kern_im + freq_im * kern_re,
            )
            wave_re, wave_im = transform(freq_re, freq_im, cosine, sine, 1.0)
    far_re, far_im = transform(wave_re, wave_im, cosine, sine, -1.0)
    differ = far_re * far_re + far_im * far_im - measured
    return weight * jnp.sum(differ * differ)


def general(object_slices, probe, intensities, row_offsets, column_starts, slice_shifts, counts):
    band = object_slices.shape[2]
    framed = padded(object_slices, (("scan", 2),), band)
    region = lax.all_gather(framed, "angle", axis=3, tiled=True)
    size = probe.shape[1]
    slots = row_offsets.shape[2]
    layers = region.shape[1]
    angles = lax.axis_size("angle")
    cosine, sine = tables(size)
    kern_re, kern_im = propagator(size)
    shifts = slice_shifts[0]
    zero = jnp.zeros((), jnp.int32)

    def visit(slot, carry):
        gradient_region, gradient_probe = carry
        top = row_offsets[0, 0, slot]
        start = column_starts[0, 0, slot]
        slab = jnp.concatenate(
            [
                lax.dynamic_slice(
                    region, (zero, zero + k, top, start + shifts[k]), (2, 1, size, size)
                )
                for k in range(layers)
            ],
            axis=1,
        )
        weight = jnp.where(slot < counts[0, 0], 0.5 / angles, 0.0).astype(jnp.float32)
        measured = intensities[0, 0, slot]
        scorer = partial(
            local_loss,
            measured=measured,
            weight=weight,
            cosine=cosine,
            sine=sine,
            kern_re=kern_re,
            kern_im=kern_im,
        )
        loss, pull = jax.vjp(scorer, slab, probe)
        slab_grad, probe_grad = pull(jnp.ones_like(loss))
        for k in range(layers):
            place = (zero, zero + k, top, start + shifts[k])
            current = lax.dynamic_slice(gradient_region, place, (2, 1, size, size))
            gradient_region = lax.dynamic_update_slice(
                gradient_region, current + slab_grad[:, k : k + 1], place
            )
        return (gradient_region, gradient_probe + probe_grad)

    start_carry = (jnp.zeros(region.shape, jnp.float32), jnp.zeros(probe.shape, jnp.float32))
    gradient_region, gradient_probe = lax.fori_loop(0, slots, visit, start_carry)
    shared = lax.psum_scatter(gradient_region, "angle", scatter_dimension=3, tiled=True)
    edges = jnp.concatenate([shared[:, :, :band], shared[:, :, 2 * band :]], axis=2)
    rimmed = padded(edges, (("scan", 2),), band)
    object_gradient = shared[:, :, band : 2 * band] + rimmed[:, :, :band] + rimmed[:, :, 3 * band :]
    group_total = lax.psum(gradient_probe, "scan")
    probe_gradient = lax.psum(group_total, "angle")
    return (object_gradient, probe_gradient)


def packable(object_slices, probe):
    size = probe.shape[1]
    band, width = object_slices.shape[2:]
    return 2 * width == size == 128 and band % 8 == 0 and lax.axis_size("angle") == 2**3


def local(object_slices, probe, intensities, row_offsets, column_starts, slice_shifts, counts):
    args = (object_slices, probe, intensities, row_offsets, column_starts, slice_shifts, counts)
    if not packable(object_slices, probe):
        return general(*args)
    region = gather(object_slices)
    grad, probe_grad = gradients(
        region, probe, intensities, row_offsets, column_starts, slice_shifts, counts
    )
    return reduce(grad, probe_grad)


def solution(mesh):
    return jax.shard_map(
        local,
        mesh=mesh,
        in_specs=(
            P(None, None, "scan", "angle"),
            P(),
            P("angle", "scan", None, None, None),
            P("angle", "scan", None),
            P("angle", "scan", None),
            P("angle", None),
            P("angle", "scan"),
        ),
        out_specs=(P(None, None, "scan", "angle"), P()),
        check_vma=False,
    )
```
